32 devices in a mesh: clients: 8 (over z, x), shard: 4 (over y, core).
Axes of the slice: x: 2, y: 2, z: 4, core: 2. Of those that a mesh axis runs over, the one named last changes fastest.
Arguments:
- quantized: int32 [8, 2097152], P('clients', 'shard'), may hold values from 0 to 2097151
- pair_masks: int32 [8, 2097152], P('clients', 'shard'), may hold values from 0 to 2097142, as said below
- alive_flags: int32 [8], P('clients'), may hold values from 0 to 1, as said below
- row_seeds: int32 [64], replicated, may hold values from 0 to 1073741823
Outputs:
- aggregate: int32 [2097152], P('shard')
- commitments: int32 [8, 64], P('clients')
- mismatch: int32 [64], replicated
The draws below stay inside these ranges and needn't reach their ends.
Inputs may be any that keep to these rules, and one draw needn't show every extreme that they name: For every position, the pair_masks of all 8 participants sum to a multiple of 2097143. `alive_flags`: at least one participant has flag 1 and at least one has flag 0.
All inputs are finite; a program needn't handle non-finite values.
Results may differ from the reference program's by a relative error of at most 0.000001.
Values may be sent and summed in bfloat16 or wider, within the bound.
No kernel may reach another device: no remote copies, remote signals or barrier semaphores. Data moves between devices by JAX's collectives and lax.ppermute only.
A program may use at most 64 MiB of HBM per device.

```python
import math
import jax
import jax.numpy as jnp
from jax import lax

ROWS = 64
CLIENTS = 8
L = 2097152


def draw_pair_masks(key, part):
    drawn_base = jax.random.randint(jax.random.fold_in(key, 11), (CLIENTS, L), 0, 2097143, dtype=jnp.int32)
    following = jnp.roll(drawn_base, -1, axis=0)
    return (drawn_base - following) % 2097143


def draw_alive_flags(key, part):
    drawn_bits = jax.random.randint(jax.random.fold_in(key, 23), (CLIENTS,), 0, 2, dtype=jnp.int32)
    chosen = jax.random.randint(jax.random.fold_in(key, 29), (), 0, CLIENTS, dtype=jnp.int32)
    position = jnp.arange(CLIENTS, dtype=jnp.int32)
    drawn_bits = jnp.where(position == chosen, 0, drawn_bits)
    return jnp.where(position == (chosen + 1) % CLIENTS, 1, drawn_bits).astype(jnp.int32)


def with_ends(values, rng, least, largest):
    longest = values.shape.index(max(values.shape))
    spots = []
    for shift in (0, 1):
        where = [jax.random.randint(jax.random.fold_in(rng, axis), (), 0, length) for axis, length in enumerate(values.shape)]
        where[longest] = (where[longest] + shift) % values.shape[longest]
        spots.append(tuple(where))
    return values.at[spots[0]].set(least).at[spots[1]].set(largest)


def setup_inputs(seed: int = 0) -> dict:
    seeds = jax.random.split(jax.random.key(seed), 5)
    quantized = with_ends(jax.random.randint(seeds[0], (CLIENTS, L), 0, 2097152), jax.random.fold_in(seeds[0], 1), 0, 2097151).astype(jnp.int32)
    pair_masks = draw_pair_masks(jax.random.fold_in(seeds[4], 71), 0)
    alive_flags = draw_alive_flags(jax.random.fold_in(seeds[4], 71), 0)
    row_seeds = with_ends(jax.random.randint(seeds[3], (ROWS,), 0, 1073741824), jax.random.fold_in(seeds[3], 1), 0, 1073741823).astype(jnp.int32)
    return dict(quantized=quantized, pair_masks=pair_masks, alive_flags=alive_flags, row_seeds=row_seeds)


modulus = 2097143


def table_entries(row_seeds, columns):
    mixed = columns[None, :] * 747796405 + row_seeds[:, None]
    mixed = mixed & 2147483647
    mixed = mixed ^ (mixed >> 15)
    mixed = (mixed * 277803737) & 2147483647
    mixed = mixed ^ (mixed >> 13)
    mixed = (mixed * 1103515245) & 2147483647
    mixed = mixed ^ (mixed >> 16)
    return mixed & 1023


def project_mod(row_seeds, vectors, offset, block_width):
    vec_count = vectors.shape[0]
    length = vectors.shape[1]
    row_count = row_seeds.shape[0]
    sub_width = math.gcd(block_width, 512)
    block_count = length // block_width

    def advance(running, block_index):
        start_col = block_index * block_width
        columns = offset + start_col + jnp.arange(block_width, dtype=jnp.int32)
        table = table_entries(row_seeds, columns)
        right_part = lax.dynamic_slice_in_dim(vectors, start_col, block_width, 1)
        products = (right_part[:, None, :] * table[None, :, :]) % modulus
        products = products.reshape(vec_count, row_count, block_width // sub_width, sub_width)
        partial_value = jnp.sum(products, axis=3, dtype=jnp.int32) % modulus
        partial_value = jnp.sum(partial_value, axis=2, dtype=jnp.int32) % modulus
        return (running + partial_value) % modulus, None

    running = jnp.zeros((vec_count, row_count), jnp.int32)
    running, unused = lax.scan(advance, running, jnp.arange(block_count, dtype=jnp.int32))
    return running


def reference(quantized, pair_masks, alive_flags, row_seeds):
    masked = ((quantized + pair_masks) % modulus) * alive_flags[:, None]
    aggregate = jnp.sum(masked, axis=0, dtype=jnp.int32) % modulus
    col_block = math.gcd(quantized.shape[1], 4096)
    commitments = project_mod(row_seeds, quantized, 0, col_block)
    expected = jnp.sum(commitments * alive_flags[:, None], axis=0, dtype=jnp.int32) % modulus
    projected = project_mod(row_seeds, aggregate[None, :], 0, col_block)[0]
    mismatch = (projected - expected) % modulus
    return aggregate, commitments, mismatch
```

```python
import functools

import jax
import jax.numpy as jnp
from jax import lax
from jax.experimental import pallas as pl
from jax.experimental.pallas import tpu as pltpu
from jax.sharding import PartitionSpec as P


modulus = 2097143
lanes = 128
tile = 8 * lanes
low_bits = 11
low_mask = (1 << low_bits) - 1
stride = (tile * 747796405 + (1 << 31)) % (1 << 32) - (1 << 31)


def mod_once(value):
    return jnp.where(value >= modulus, value - modulus, value)


def entries(value):
    value = value & 2147483647
    value = value ^ (value >> 15)
    value = (value * 277803737) & 2147483647
    value = value ^ (value >> 13)
    value = value * 1103515245
    return (value ^ (value >> 16)) & 1023


def project_kernel(seeds_ref, start_ref, vec_ref, out_ref, base_ref, low_ref, high_ref, sum_ref, *, row_block, unroll):
    steps = vec_ref.shape[0] // 8
    spot = lax.broadcasted_iota(jnp.int32, (8, lanes), 0) * lanes + lax.broadcasted_iota(jnp.int32, (8, lanes), 1)
    block_index = pl.program_id(0)
    first = (spot + start_ref[0] + block_index * (steps * tile)) * 747796405

    def prepare(step, carry):
        at = pl.ds(pl.multiple_of(step * 8, 8), 8)
        value = vec_ref[at, :]
        base_ref[at, :] = first + step * stride
        low_ref[at, :] = value & low_mask
        high_ref[at, :] = value >> low_bits
        return carry

    lax.fori_loop(0, steps, prepare, 0, unroll=4)

    def rows(block, carry):
        seeds = [jnp.full((8, lanes), seeds_ref[block * row_block + r], jnp.int32) for r in range(row_block)]

        def columns(step, sums):
            at = pl.ds(pl.multiple_of(step * 8, 8), 8)
            base, low, high = base_ref[at, :], low_ref[at, :], high_ref[at, :]
            out = []
            for r in range(row_block):
                table = entries(base + seeds[r])
                out.append(sums[2 * r] + table * low)
                out.append(sums[2 * r + 1] + table * high)
            return tuple(out)

        zero = jnp.zeros((8, lanes), jnp.int32)
        sums = [jnp.where(block_index == 0, zero, sum_ref[block * row_block + i // 2, i % 2]) for i in range(2 * row_block)]
        sums = lax.fori_loop(0, steps, columns, tuple(sums), unroll=unroll)
        for r in range(row_block):
            for part in range(2):
                sum_ref[block * row_block + r, part] = sums[2 * r + part]
        return carry

    lax.fori_loop(0, sum_ref.shape[0] // row_block, rows, 0)

    @pl.when(block_index == pl.num_programs(0) - 1)
    def finish():
        for part in range(2):
            sums = sum_ref[:, part]
            out_ref[part, 0] = jnp.sum(sums & 65535, axis=1)
            out_ref[part, 1] = jnp.sum(sums >> 16, axis=1)


def project(row_seeds, vector, start, height, low, high):
    rows = row_seeds.shape[0]
    assert height % 8 == 0 and (high - low) * height // 8 <= 1024
    return pl.pallas_call(
        functools.partial(project_kernel, row_block=8, unroll=2),
        grid=(high - low,),
        out_shape=jax.ShapeDtypeStruct((2, 2, rows, lanes), jnp.int32),
        cost_estimate=pl.CostEstimate(flops=(high - low) * height * rows * 4096, bytes_accessed=0, transcendentals=0),
        in_specs=[
            pl.BlockSpec(memory_space=pltpu.SMEM),
            pl.BlockSpec(memory_space=pltpu.SMEM),
            pl.BlockSpec((height, lanes), lambda i: (low + i, 0)),
        ],
        out_specs=pl.BlockSpec((2, 2, rows, lanes), lambda i: (0, 0, 0, 0)),
        scratch_shapes=[pltpu.VMEM((height, lanes), jnp.int32)] * 3 + [pltpu.VMEM((rows, 2, 8, lanes), jnp.int32)],
    )(row_seeds, (start + low * height * lanes)[None], vector)

def fold(sums):
    sums = jnp.sum(sums, axis=-1) % modulus
    high = sums[..., 1, :]
    for step in range(16):
        high = mod_once(high + high)
    parts = mod_once(sums[..., 0, :] + high)
    high = parts[..., 1, :]
    for step in range(low_bits):
        high = mod_once(high + high)
    return mod_once(parts[..., 0, :] + high)


def pack(value):
    a, b, c, d = jnp.split(value, 4, axis=-2)
    return jnp.concatenate([a | (d & 127) << 21, b | (d >> 7 & 127) << 21, c | (d >> 14) << 21], axis=-2)


def unpack(value):
    a, b, c = jnp.split(value, 3, axis=-2)
    mask = 2097151
    return jnp.concatenate([a & mask, b & mask, c & mask, (a >> 21) | (b >> 21) << 7 | (c >> 21) << 14], axis=-2)


def body(quantized, pair_masks, alive_flags, row_seeds):
    alive = alive_flags[0]
    length = quantized.shape[1]
    clients = lax.axis_size("clients")
    shards = lax.axis_size("shard")
    me = lax.axis_index("clients")
    offset = lax.axis_index("shard") * length
    outer = clients // 2
    inner_index = me % 2
    outer_index = me // 2
    height = length // lanes
    share = height // clients

    q = quantized.reshape(height, lanes)
    m = pair_masks.reshape(height, lanes)
    masked = mod_once(mod_once(q + m)) * alive
    pieces = masked.reshape(2, outer, share, lanes)

    def swap(value):
        return lax.ppermute(value, "clients", [(c, c ^ 1) for c in range(clients)])

    def shift(value, by):
        return lax.ppermute(
            value, "clients", [(c, ((c // 2 + by) % outer) * 2 + c % 2) for c in range(clients)]
        )

    keep = lax.dynamic_index_in_dim(pieces, inner_index, 0, keepdims=False)
    give = lax.dynamic_index_in_dim(pieces, 1 - inner_index, 0, keepdims=False)
    got = swap(pack(give))
    cuts = [0, 3, 6, 8]

    def part(index, vector):
        return project(row_seeds, vector, offset, height // cuts[-1], cuts[index], cuts[index + 1])

    first = part(0, q)
    q, got, first = lax.optimization_barrier((q, got, first))
    half = mod_once(keep + unpack(got))
    sent = [
        pack(lax.dynamic_index_in_dim(half, (outer_index + by) % outer, 0, keepdims=False)) for by in range(1, outer)
    ]
    q, sent = lax.optimization_barrier((q, sent))
    sent = [shift(value, by) for by, value in enumerate(sent, 1)]
    second = part(1, q)
    q, sent, second = lax.optimization_barrier((q, sent, second))
    own = lax.dynamic_index_in_dim(half, outer_index, 0, keepdims=False)
    for value in sent:
        own = own + unpack(value)
    own = own % modulus
    q, own, packed = lax.optimization_barrier((q, own, pack(own)))
    taken = [shift(packed, by) for by in range(1, outer)]
    piece_start = offset + (inner_index * outer + outer_index) * share * lanes
    third = part(2, q)
    projected = project(row_seeds, own, piece_start, share, 0, 1)
    taken, third, projected = lax.optimization_barrier((taken, third, projected))
    column = jnp.zeros((outer,) + packed.shape, jnp.int32)
    column = lax.dynamic_update_index_in_dim(column, packed, outer_index, 0)
    for by, value in enumerate(taken, 1):
        column = lax.dynamic_update_index_in_dim(column, value, (outer_index - by) % outer, 0)
    other = swap(column)
    mine, projected = fold(jnp.stack([first + second + third, projected]))

    note = jnp.concatenate([mine, mine * alive, projected])
    devices = clients * shards
    notes = lax.all_to_all(
        jnp.broadcast_to(note, (devices, note.shape[0])), ("clients", "shard"), 0, 0, tiled=True
    ).reshape(clients, shards, 3, row_seeds.shape[0])
    commitments = jnp.sum(lax.dynamic_index_in_dim(notes[:, :, 0], me, 0, keepdims=False), axis=0) % modulus
    expected = jnp.sum(notes[:, :, 1], axis=(0, 1)) % modulus
    total = jnp.sum(notes[:, :, 2], axis=(0, 1)) % modulus
    mismatch = jnp.where(total >= expected, total - expected, total - expected + modulus)

    whole = jnp.stack([jnp.where(inner_index == 0, column, other), jnp.where(inner_index == 0, other, column)])
    aggregate = unpack(whole).reshape(length)
    return (aggregate, commitments[None, :], mismatch)


def solution(mesh):
    placed = (P("clients", "shard"), P("clients", "shard"), P("clients"), P())
    return jax.shard_map(
        body,
        mesh=mesh,
        in_specs=placed,
        out_specs=(P("shard"), P("clients", None), P()),
        check_vma=False,
    )
```

```python
import jax
import jax.numpy as jnp
from jax import lax
from jax.experimental import pallas as pl
from jax.experimental.pallas import tpu as pltpu
from jax.sharding import PartitionSpec as P


modulus = 2097143
lanes = 128
group = 4
vectors = 8
chunk = 2048
strip = lanes


def mod_once(value):
    return jnp.where(value >= modulus, value - modulus, value)


def entries(value):
    value = value & 2147483647
    value = value ^ (value >> 15)
    value = (value * 277803737) & 2147483647
    value = value ^ (value >> 13)
    value = value * 1103515245
    return value ^ (value >> 16)


def project_kernel(starts_ref, seeds_ref, vec_ref, out_ref):
    block_index = pl.program_id(0)
    start = starts_ref[block_index]

    @pl.when(block_index == 0)
    def clear():
        out_ref[...] = jnp.zeros(out_ref.shape, jnp.int32)

    seeds = seeds_ref[...]
    spot = lax.broadcasted_iota(jnp.int32, (8, chunk), 1)[:1]

    def part(value):
        return value.astype(jnp.float32).astype(jnp.bfloat16)

    def columns(step, sums):
        at = pl.multiple_of(step * chunk, chunk)
        base = (spot + (start + at)) * 747796405
        strips = []
        for low in range(0, chunk, strip):
            table = entries(base[:, low : low + strip] + seeds)
            strips.append(jnp.concatenate([part(table & 31), part((table >> 5) & 31)], axis=0))
        value = vec_ref[:, pl.ds(at, chunk)]
        value = jnp.concatenate([value & 127, (value >> 7) & 127, value >> 14], axis=0)
        product = lax.dot_general(
            part(value),
            jnp.concatenate(strips, axis=1),
            (((1,), (1,)), ((), ())),
            preferred_element_type=jnp.float32,
        )
        return sums + product.astype(jnp.int32)

    steps = vec_ref.shape[1] // chunk
    out_ref[...] += lax.fori_loop(0, steps, columns, jnp.zeros(out_ref.shape, jnp.int32))


def project(seeds, vector, starts, which):
    rows = seeds.shape[0]
    blocks = starts.shape[0]
    width = vector.shape[1] // blocks // 2
    assert width % chunk == 0 and vector.shape[1] <= 1 << 19
    return pl.pallas_call(
        project_kernel,
        grid=(blocks,),
        out_shape=jax.ShapeDtypeStruct((3 * vectors, 2 * rows), jnp.int32),
        cost_estimate=pl.CostEstimate(flops=vector.shape[1] * rows * 1024, bytes_accessed=0, transcendentals=0),
        in_specs=[
            pl.BlockSpec(memory_space=pltpu.SMEM),
            pl.BlockSpec((rows, strip), lambda i: (0, 0)),
            pl.BlockSpec((vectors, width), lambda i: (0, 2 * i + which)),
        ],
        out_specs=pl.BlockSpec((3 * vectors, 2 * rows), lambda i: (0, 0)),
    )(starts + which * width, seeds, vector)


def fold(sums):
    sums = (sums % modulus).reshape(3, vectors, 2, -1)
    sums = (sums[:, :, 0] + sums[:, :, 1] * 32) % modulus
    return (sums[0] + (sums[1] + sums[2] * 128 % modulus) % modulus * 128) % modulus


def pack(value):
    a, b, c, d = jnp.split(value, 4, axis=-2)
    return jnp.concatenate([a | (d & 127) << 21, b | (d >> 7 & 127) << 21, c | (d >> 14) << 21], axis=-2)


def unpack(value):
    a, b, c = jnp.split(value, 3, axis=-2)
    mask = 2097151
    return jnp.concatenate([a & mask, b & mask, c & mask, (a >> 21) | (b >> 21) << 7 | (c >> 21) << 14], axis=-2)


def body(quantized, pair_masks, alive_flags, row_seeds):
    alive = alive_flags[0]
    length = quantized.shape[1]
    clients = lax.axis_size("clients")
    shards = lax.axis_size("shard")
    me = lax.axis_index("clients")
    offset = lax.axis_index("shard") * length
    rows = row_seeds.shape[0]
    outer = clients // 2
    upper = clients // group
    inner_index = me % 2
    outer_index = me // 2
    middle_index = outer_index % 2
    upper_index = me // group
    height = length // lanes
    share = height // clients
    width = share * lanes

    q = quantized.reshape(height, lanes)
    m = pair_masks.reshape(height, lanes)
    masked = mod_once(mod_once(q + m)) * alive
    pieces = masked.reshape(2, outer, share, lanes)
    q_pieces = q.reshape(2, upper, 2, share, lanes)

    def swap(value, by=1):
        return lax.ppermute(value, "clients", [(c, c ^ by) for c in range(clients)])

    def shift(value, by):
        return lax.ppermute(
            value, "clients", [(c, ((c // 2 + by) % outer) * 2 + c % 2) for c in range(clients)]
        )

    def quarter(by):
        return lax.dynamic_slice(
            q_pieces,
            (inner_index ^ (by & 1), 0, middle_index ^ (by >> 1), 0, 0),
            (1, upper, 1, share, lanes),
        )[0, :, 0]

    def piece_start(index):
        return offset + (inner_index * outer + index * 2 + middle_index) * width

    def at_outer(value, index):
        return lax.dynamic_index_in_dim(value, index, 1, keepdims=False)

    handed = [pack(quarter(by)) for by in range(1, group)]
    theirs = [swap(value, by) for by, value in enumerate(handed, 1)]
    sent = [shift(pack(at_outer(pieces, (outer_index + by) % outer)), by) for by in range(1, outer)]
    mine = jnp.stack([quarter(0)] + [unpack(value) for value in theirs]).reshape(group, upper, width)
    others = [(upper_index + by) % upper for by in range(1, upper)]
    far = jnp.concatenate([at_outer(mine, index) for index in others], axis=1)
    far = jnp.pad(far, ((0, vectors - group), (0, 0)))
    far_starts = jnp.stack([piece_start(index) for index in others])
    seeds = jnp.broadcast_to(row_seeds[:, None], (rows, strip))

    both = at_outer(pieces, outer_index)
    for value in sent:
        both = both + unpack(value)
    both = both % modulus
    give = pack(lax.dynamic_index_in_dim(both, 1 - inner_index, 0, keepdims=False))
    far, give = lax.optimization_barrier((far, give))
    got = swap(give)
    sums = project(seeds, far, far_starts, 0)

    sums, got, far = lax.optimization_barrier((sums, got, far))
    own = mod_once(lax.dynamic_index_in_dim(both, inner_index, 0, keepdims=False) + unpack(got))
    packed = pack(own)
    cut = packed.shape[0] // 3 * 2
    top, low = packed[:cut], packed[cut:]
    top, low, far = lax.optimization_barrier((top, low, far))
    low_other = swap(low)
    taken = [shift(top, by) for by in range(1, outer)]
    sums = sums + project(seeds, far, far_starts, 1)

    near = at_outer(mine, upper_index)
    near = jnp.concatenate([near, own.reshape(1, width), jnp.zeros((vectors - group - 1, width), jnp.int32)])
    near_start = piece_start(upper_index)[None]
    sums, low_other, near = lax.optimization_barrier((sums, low_other, near))
    low_both = jnp.where(inner_index == 0, jnp.stack([low, low_other]), jnp.stack([low_other, low]))
    low_both, near = lax.optimization_barrier((low_both, near))
    low_taken = [shift(low_both, by) for by in range(1, outer)]
    sums = sums + project(seeds, near, near_start, 0)

    def ordered(own_value, values):
        placed = jnp.zeros((outer,) + own_value.shape, jnp.int32)
        for by, value in enumerate([own_value] + values):
            placed = lax.dynamic_update_index_in_dim(placed, value, (outer_index - by) % outer, 0)
        return placed

    sums, taken, near = lax.optimization_barrier((sums, taken, near))
    column = ordered(top, taken)
    column, near = lax.optimization_barrier((column, near))
    other = swap(column)
    sums = sums + project(seeds, near, near_start, 1)
    parts = fold(sums)[: group + 1]
    note = jnp.concatenate([parts.reshape(-1), jnp.full((rows,), alive, jnp.int32)])

    devices = clients * shards
    notes = lax.all_to_all(
        jnp.broadcast_to(note, (devices, note.shape[0])), ("clients", "shard"), 0, 0, tiled=True
    ).reshape(clients, shards, group + 2, rows)
    notes = jnp.sum(notes, axis=1)
    everyone = [[notes[c ^ by, by] for by in range(group)] for c in range(clients)]
    everyone = jnp.stack([sum(parts) for parts in everyone]) % modulus
    commitments = lax.dynamic_index_in_dim(everyone, me, 0, keepdims=False)
    flags = notes[:, group + 1] // shards
    expected = jnp.sum(everyone * flags, axis=0) % modulus
    total = jnp.sum(notes[:, group], axis=0) % modulus
    mismatch = jnp.where(total >= expected, total - expected, total - expected + modulus)

    tops = jnp.where(inner_index == 0, jnp.stack([column, other]), jnp.stack([other, column]))
    lows = jnp.swapaxes(ordered(low_both, low_taken), 0, 1)
    aggregate = unpack(jnp.concatenate([tops, lows], axis=2)).reshape(length)
    return (aggregate, commitments[None, :], mismatch)


def solution(mesh):
    placed = (P("clients", "shard"), P("clients", "shard"), P("clients"), P())
    return jax.shard_map(
        body,
        mesh=mesh,
        in_specs=placed,
        out_specs=(P("shard"), P("clients", None), P()),
        check_vma=False,
    )
```

```python
import jax
import jax.numpy as jnp
from jax import lax
from jax.experimental import pallas as pl
from jax.experimental.pallas import tpu as pltpu
from jax.sharding import PartitionSpec as P


modulus = 2097143
lanes = 128
group = 4
vectors = 8
chunk = 2048
strip = lanes


def mod_once(value):
    return jnp.where(value >= modulus, value - modulus, value)


def entries(value):
    value = value & 2147483647
    value = value ^ (value >> 15)
    value = (value * 277803737) & 2147483647
    value = value ^ (value >> 13)
    value = value * 1103515245
    return value ^ (value >> 16)


def project_kernel(starts_ref, seeds_ref, vec_ref, out_ref):
    block_index = pl.program_id(0)
    start = starts_ref[block_index]

    @pl.when(block_index == 0)
    def clear():
        out_ref[...] = jnp.zeros(out_ref.shape, jnp.int32)

    seeds = seeds_ref[...]
    spot = lax.broadcasted_iota(jnp.int32, (8, chunk), 1)[:1]

    def part(value):
        return value.astype(jnp.float32).astype(jnp.bfloat16)

    def columns(step, sums):
        at = pl.multiple_of(step * chunk, chunk)
        base = (spot + (start + at)) * 747796405
        strips = []
        for low in range(0, chunk, strip):
            table = entries(base[:, low : low + strip] + seeds)
            strips.append(jnp.concatenate([part(table & 31), part((table >> 5) & 31)], axis=0))
        value = vec_ref[:, pl.ds(at, chunk)]
        value = jnp.concatenate([value & 127, (value >> 7) & 127, value >> 14], axis=0)
        product = lax.dot_general(
            part(value),
            jnp.concatenate(strips, axis=1),
            (((1,), (1,)), ((), ())),
            preferred_element_type=jnp.float32,
        )
        return sums + product.astype(jnp.int32)

    steps = vec_ref.shape[1] // chunk
    out_ref[...] += lax.fori_loop(0, steps, columns, jnp.zeros(out_ref.shape, jnp.int32))


def project(seeds, vector, starts, which):
    rows = seeds.shape[0]
    blocks = starts.shape[0]
    width = vector.shape[1] // blocks // 2
    assert width % chunk == 0 and vector.shape[1] <= 1 << 19
    return pl.pallas_call(
        project_kernel,
        grid=(blocks,),
        out_shape=jax.ShapeDtypeStruct((3 * vectors, 2 * rows), jnp.int32),
        cost_estimate=pl.CostEstimate(flops=vector.shape[1] * rows * 1024, bytes_accessed=0, transcendentals=0),
        in_specs=[
            pl.BlockSpec(memory_space=pltpu.SMEM),
            pl.BlockSpec((rows, strip), lambda i: (0, 0)),
            pl.BlockSpec((vectors, width), lambda i: (0, 2 * i + which)),
        ],
        out_specs=pl.BlockSpec((3 * vectors, 2 * rows), lambda i: (0, 0)),
    )(starts + which * width, seeds, vector)


def fold(sums):
    sums = (sums % modulus).reshape(3, vectors, 2, -1)
    sums = (sums[:, :, 0] + sums[:, :, 1] * 32) % modulus
    return (sums[0] + (sums[1] + sums[2] * 128 % modulus) % modulus * 128) % modulus


def pack(value):
    a, b, c, d = jnp.split(value, 4, axis=-2)
    return jnp.concatenate([a | (d & 127) << 21, b | (d >> 7 & 127) << 21, c | (d >> 14) << 21], axis=-2)


def unpack(value):
    a, b, c = jnp.split(value, 3, axis=-2)
    mask = 2097151
    return jnp.concatenate([a & mask, b & mask, c & mask, (a >> 21) | (b >> 21) << 7 | (c >> 21) << 14], axis=-2)


def body(quantized, pair_masks, alive_flags, row_seeds):
    alive = alive_flags[0]
    length = quantized.shape[1]
    clients = lax.axis_size("clients")
    shards = lax.axis_size("shard")
    me = lax.axis_index("clients")
    offset = lax.axis_index("shard") * length
    rows = row_seeds.shape[0]
    outer = clients // 2
    upper = clients // group
    inner_index = me % 2
    outer_index = me // 2
    middle_index = outer_index % 2
    upper_index = me // group
    height = length // lanes
    share = height // clients
    width = share * lanes

    q = quantized.reshape(height, lanes)
    m = pair_masks.reshape(height, lanes)
    q_pieces = q.reshape(2, upper, 2, share, lanes)

    def swap(value, by=1):
        return lax.ppermute(value, "clients", [(c, c ^ by) for c in range(clients)])

    def shift(value, by):
        return lax.ppermute(
            value, "clients", [(c, ((c // 2 + by) % outer) * 2 + c % 2) for c in range(clients)]
        )

    def quarter(by):
        return lax.dynamic_slice(
            q_pieces,
            (inner_index ^ (by & 1), 0, middle_index ^ (by >> 1), 0, 0),
            (1, upper, 1, share, lanes),
        )[0, :, 0]

    def piece_start(index):
        return offset + (inner_index * outer + index * 2 + middle_index) * width

    def at_outer(value, index):
        return lax.dynamic_index_in_dim(value, index, 1, keepdims=False)

    handed = [pack(quarter(by)) for by in range(1, group)]
    handed, m = lax.optimization_barrier((handed, m))
    masked = mod_once(mod_once(q + m)) * alive
    pieces = masked.reshape(2, outer, share, lanes)
    theirs = [swap(value, by) for by, value in enumerate(handed, 1)]
    sent = [shift(pack(at_outer(pieces, (outer_index + by) % outer)), by) for by in range(1, outer)]
    mine = jnp.stack([quarter(0)] + [unpack(value) for value in theirs]).reshape(group, upper, width)
    others = [(upper_index + by) % upper for by in range(1, upper)]
    far = jnp.concatenate([at_outer(mine, index) for index in others], axis=1)
    far = jnp.pad(far, ((0, vectors - group), (0, 0)))
    far_starts = jnp.stack([piece_start(index) for index in others])
    seeds = jnp.broadcast_to(row_seeds[:, None], (rows, strip))

    both = at_outer(pieces, outer_index)
    for value in sent:
        both = both + unpack(value)
    both = both % modulus
    give = pack(lax.dynamic_index_in_dim(both, 1 - inner_index, 0, keepdims=False))
    far, give = lax.optimization_barrier((far, give))
    got = swap(give)
    sums = project(seeds, far, far_starts, 0)

    sums, got, far = lax.optimization_barrier((sums, got, far))
    own = mod_once(lax.dynamic_index_in_dim(both, inner_index, 0, keepdims=False) + unpack(got))
    packed = pack(own)
    cut = packed.shape[0] // 3 * 2
    top, low = packed[:cut], packed[cut:]
    top, low, far = lax.optimization_barrier((top, low, far))
    low_other = swap(low)
    taken = [shift(top, by) for by in range(1, outer)]
    sums = sums + project(seeds, far, far_starts, 1)

    near = at_outer(mine, upper_index)
    near = jnp.concatenate([near, own.reshape(1, width), jnp.zeros((vectors - group - 1, width), jnp.int32)])
    near_start = piece_start(upper_index)[None]
    sums, low_other, near = lax.optimization_barrier((sums, low_other, near))
    low_both = jnp.where(inner_index == 0, jnp.stack([low, low_other]), jnp.stack([low_other, low]))
    low_both, near = lax.optimization_barrier((low_both, near))
    low_taken = [shift(low_both, by) for by in range(1, outer)]
    sums = sums + project(seeds, near, near_start, 0)

    def ordered(own_value, values):
        placed = jnp.zeros((outer,) + own_value.shape, jnp.int32)
        for by, value in enumerate([own_value] + values):
            placed = lax.dynamic_update_index_in_dim(placed, value, (outer_index - by) % outer, 0)
        return placed

    sums, taken, near = lax.optimization_barrier((sums, taken, near))
    column = ordered(top, taken)
    column, near = lax.optimization_barrier((column, near))
    other = swap(column)
    sums = sums + project(seeds, near, near_start, 1)
    parts = fold(sums)[: group + 1]
    note = jnp.concatenate([parts.reshape(-1), jnp.full((rows,), alive, jnp.int32)])

    devices = clients * shards
    notes = lax.all_to_all(
        jnp.broadcast_to(note, (devices, note.shape[0])), ("clients", "shard"), 0, 0, tiled=True
    ).reshape(clients, shards, group + 2, rows)
    notes = jnp.sum(notes, axis=1)
    everyone = [[notes[c ^ by, by] for by in range(group)] for c in range(clients)]
    everyone = jnp.stack([sum(parts) for parts in everyone]) % modulus
    commitments = lax.dynamic_index_in_dim(everyone, me, 0, keepdims=False)
    flags = notes[:, group + 1] // shards
    expected = jnp.sum(everyone * flags, axis=0) % modulus
    total = jnp.sum(notes[:, group], axis=0) % modulus
    mismatch = jnp.where(total >= expected, total - expected, total - expected + modulus)

    tops = jnp.where(inner_index == 0, jnp.stack([column, other]), jnp.stack([other, column]))
    lows = jnp.swapaxes(ordered(low_both, low_taken), 0, 1)
    aggregate = unpack(jnp.concatenate([tops, lows], axis=2)).reshape(length)
    return (aggregate, commitments[None, :], mismatch)


def solution(mesh):
    placed = (P("clients", "shard"), P("clients", "shard"), P("clients"), P())
    return jax.shard_map(
        body,
        mesh=mesh,
        in_specs=placed,
        out_specs=(P("shard"), P("clients", None), P()),
        check_vma=False,
    )
```
